32 devices in a mesh: sp: 16 (over z, x, core), dp: 2 (over y).
Axes of the slice: x: 2, y: 2, z: 4, core: 2. Of those that a mesh axis runs over, the one named last changes fastest.
Arguments:
- queries: bfloat16 [1536, 24, 128], P(('dp', 'sp')), parts along dimension 0, may hold values from -12 to 12
- keys: bfloat16 [1536, 24, 128], P(('dp', 'sp')), parts along dimension 0, may hold values from -6 to 6
- values: bfloat16 [1536, 24, 128], P(('dp', 'sp')), parts along dimension 0, may hold values from -6 to 6
Outputs:
- attended: bfloat16 [1536, 3072], P(('dp', 'sp')), parts along dimension 0
The draws below stay inside these ranges and needn't reach their ends.
There are 2 independent parts, one for each index of `dp`. The reference program is written for one: setup_inputs(seed, part) draws one part's arguments, and reference() takes and returns one part's arrays. A program takes and returns all parts, laid end to end along the dimension named above; each array names one. Nothing has to cross between parts.
All inputs are finite; a program needn't handle non-finite values.
Results may differ from the reference program's by a relative error of at most 0.0049.
Values may be sent and summed in bfloat16 or wider, within the bound.
A program may use at most 64 MiB of HBM per device.

```python
import jax
import jax.numpy as jnp
from jax import lax

HEADS = 24
HEAD_DIM = 128
SEQ = 768


def draw_queries(key, part):
    own_key = jax.random.fold_in(key, 1)
    result = 2.5 * jax.random.truncated_normal(own_key, -4.8, 4.8, (SEQ, HEADS, HEAD_DIM), jnp.float32)
    return result.astype(jnp.bfloat16)


def draw_keys(key, part):
    own_key = jax.random.fold_in(key, 2)
    result = jax.random.truncated_normal(own_key, -6.0, 6.0, (SEQ, HEADS, HEAD_DIM), jnp.float32)
    return result.astype(jnp.bfloat16)


def levels(rng, extent, pieces, least, largest):
    level, own = 1.0, jax.random.fold_in(rng, 6)
    for position, shards_of in pieces:
        steps = jnp.exp(jax.random.uniform(jax.random.fold_in(own, position), (shards_of,), jnp.float32, least / len(pieces), largest / len(pieces)))
        level = level * jnp.repeat(steps, extent[position] // shards_of).reshape([-1 if axis == position else 1 for axis in range(len(extent))])
    return level


def gaussian(stream_key, shape, scale, bound, pieces=(), dtype=jnp.bfloat16):
    drawn = jax.random.normal(stream_key, shape, jnp.float32) * scale
    if len(pieces) > 0:
        drawn = levels(stream_key, shape, pieces, -0.22, 0.18) * drawn
    return jnp.clip(drawn, min=-bound, max=bound).astype(dtype)


def setup_inputs(seed: int = 0, part: int = 0) -> dict:
    splits = jax.random.split(jax.random.key(seed), 4)
    part_keys = jax.random.split(jax.random.fold_in(splits[3], part), 4)
    return {
        "queries": draw_queries(jax.random.fold_in(jax.random.fold_in(splits[3], part), 71), part),
        "keys": draw_keys(jax.random.fold_in(jax.random.fold_in(splits[3], part), 71), part),
        "values": gaussian(part_keys[2], (SEQ, HEADS, HEAD_DIM), 1.0, 6.0, ((0, 16),)),
    }


def attend(triple):
    head_q, head_k, head_v = triple
    scale = 1.0 / (head_q.shape[-1] ** 0.5)
    scores = jnp.dot(head_q, head_k.T, preferred_element_type=jnp.float32) * scale
    weights = jax.nn.softmax(scores, axis=-1).astype(jnp.bfloat16)
    return jnp.dot(weights, head_v, preferred_element_type=jnp.float32)


def reference(queries, keys, values):
    seq_len, heads, width = queries.shape
    result = lax.map(attend, (queries.transpose(1, 0, 2), keys.transpose(1, 0, 2), values.transpose(1, 0, 2)))
    return result.transpose(1, 0, 2).reshape(seq_len, heads * width).astype(jnp.bfloat16)
```

```python
import functools
import math

import jax
import jax.numpy as jnp
from jax import lax
from jax.experimental import pallas as pl
from jax.experimental.pallas import tpu as pltpu
from jax.sharding import PartitionSpec as P

HGROUPS = 8
MESH = pl.DeviceIdType.MESH


def order_of(group, groups):
    half = groups // 2
    side = group // half
    far = [(1 - side) * half + lax.rem(group + step, half) for step in range(half)]
    near = [side * half + lax.rem(group + step, half) for step in range(1, half)]
    return far + near


def kernel(
    groups, blocks, per_group,
    q_hbm, k_hbm, v_hbm, out_hbm,
    raw, wide, send, held, result, landed,
    in_sem, own_sem, send_sem, recv_sem, pass_sem, took_sem, back_sem, home_sem, out_sem,
):
    me = lax.axis_index("sp")
    group, block = me // blocks, lax.rem(me, blocks)
    tokens, heads, width = q_hbm.shape
    half = groups // 2
    others = order_of(group, groups)
    partners = [lax.rem(block + step, blocks) for step in range(1, blocks)]

    loads = [
        pltpu.make_async_copy(src, raw.at[i], in_sem.at[i])
        for i, src in enumerate((q_hbm, k_hbm, v_hbm))
    ]
    for load in loads:
        load.start()

    barrier = pltpu.get_barrier_semaphore()
    for other in others:
        pl.semaphore_signal(barrier, inc=1, device_id={"sp": other * blocks + block}, device_id_type=MESH)
    for partner in partners:
        pl.semaphore_signal(barrier, inc=1, device_id={"sp": group * blocks + partner}, device_id_type=MESH)

    for i, load in enumerate(loads):
        load.wait()
        wide[i] = raw[i].astype(jnp.float32).reshape(tokens * heads, width)

    def outward(j, other):
        return pltpu.make_async_remote_copy(
            src_ref=send.at[other, j],
            dst_ref=held.at[j, block, group],
            send_sem=send_sem.at[j, other],
            recv_sem=recv_sem.at[j, group],
            device_id={"sp": other * blocks + block},
            device_id_type=MESH,
        )

    def inward(j, other):
        return pltpu.make_async_remote_copy(
            src_ref=send.at[other, j],
            dst_ref=held.at[j, block, other],
            send_sem=send_sem.at[j, other],
            recv_sem=recv_sem.at[j, other],
            device_id={"sp": other * blocks + block},
            device_id_type=MESH,
        )

    def own(j):
        return pltpu.make_async_copy(send.at[group, j], held.at[j, block, group], own_sem.at[j])

    def share(j, source, partner):
        part = held.at[j, block, source, pl.ds(1, 2)]
        return pltpu.make_async_remote_copy(
            src_ref=part,
            dst_ref=part,
            send_sem=pass_sem.at[j, partner, source],
            recv_sem=took_sem.at[j, block, source],
            device_id={"sp": group * blocks + partner},
            device_id_type=MESH,
        )

    def shared(j, source, partner):
        part = held.at[j, partner, source, pl.ds(1, 2)]
        return pltpu.make_async_remote_copy(
            src_ref=part,
            dst_ref=part,
            send_sem=pass_sem.at[j, partner, source],
            recv_sem=took_sem.at[j, partner, source],
            device_id={"sp": group * blocks + partner},
            device_id_type=MESH,
        )

    def columns(of, j):
        return pl.ds(pl.multiple_of((of * per_group + j) * width, width), width)

    def back(j, other):
        return pltpu.make_async_remote_copy(
            src_ref=result.at[j, other],
            dst_ref=landed.at[:, columns(group, j)],
            send_sem=back_sem.at[j, other],
            recv_sem=home_sem.at[j, group],
            device_id={"sp": other * blocks + block},
            device_id_type=MESH,
        )

    def home(j, other):
        return pltpu.make_async_remote_copy(
            src_ref=result.at[j, other],
            dst_ref=landed.at[:, columns(other, j)],
            send_sem=back_sem.at[j, other],
            recv_sem=home_sem.at[j, other],
            device_id={"sp": other * blocks + block},
            device_id_type=MESH,
        )

    def own_back(j):
        return pltpu.make_async_copy(
            result.at[j, group], landed.at[:, columns(group, j)], home_sem.at[j, group]
        )

    for j in range(per_group):
        for to in range(groups):
            head = to * per_group + j
            for i in range(3):
                rows = wide[i, pl.ds(head, tokens, stride=heads), :]
                send[to, j, i] = rows.astype(jnp.bfloat16)
        if j == 0:
            pl.semaphore_wait(barrier, groups - 1 + blocks - 1)
        for other in others:
            outward(j, other).start()
        own(j).start()

    factor = math.log2(math.e) / math.sqrt(width)
    for j in range(per_group):
        own(j).wait()
        for partner in partners:
            share(j, group, partner).start()
        for other in others:
            inward(j, other).wait_recv()
            for partner in partners:
                share(j, other, partner).start()
        for partner in partners:
            for source in [group] + others:
                shared(j, source, partner).wait_recv()
        keys = held[j, :, :, 1].reshape(-1, width)
        values = held[j, :, :, 2].reshape(-1, width)
        side = group // half
        for first, picked in (((1 - side) * half, others[:half]), (side * half, others[half:])):
            queries = held[j, block, pl.ds(first, half), 0].reshape(half * tokens, width)
            scores = lax.dot_general(
                queries, keys, (((1,), (1,)), ((), ())), preferred_element_type=jnp.float32
            )
            top = jnp.max(scores, axis=-1, keepdims=True)
            weights = jnp.exp2((scores - top) * factor)
            total = jnp.sum(weights, axis=-1, keepdims=True)
            attended = jnp.dot(
                weights.astype(jnp.bfloat16), values, preferred_element_type=jnp.float32
            ) / total
            result[j, pl.ds(first, half)] = attended.astype(jnp.bfloat16).reshape(half, tokens, width)
            for other in picked:
                back(j, other).start()
        own_back(j).start()

    for j in range(per_group):
        own_back(j).wait()
        for other in others:
            home(j, other).wait_recv()
    store = pltpu.make_async_copy(landed, out_hbm, out_sem)
    store.start()
    for j in range(per_group):
        for other in others:
            outward(j, other).wait_send()
            back(j, other).wait_send()
        for partner in partners:
            for source in [group] + others:
                share(j, source, partner).wait_send()
    store.wait()


def shards(queries, keys, values):
    tokens, heads, width = queries.shape
    groups = HGROUPS
    blocks = lax.axis_size("sp") // groups
    per_group = heads // groups
    kind = queries.dtype
    return pl.pallas_call(
        functools.partial(kernel, groups, blocks, per_group),
        out_shape=jax.ShapeDtypeStruct((tokens, heads * width), kind),
        in_specs=[pl.BlockSpec(memory_space=pl.ANY)] * 3,
        out_specs=pl.BlockSpec(memory_space=pl.ANY),
        scratch_shapes=[
            pltpu.VMEM((3, tokens, heads, width), kind),
            pltpu.VMEM((3, tokens * heads, width), jnp.float32),
            pltpu.VMEM((groups, per_group, 3, tokens, width), kind),
            pltpu.VMEM((per_group, blocks, groups, 3, tokens, width), kind),
            pltpu.VMEM((per_group, groups, tokens, width), kind),
            pltpu.VMEM((tokens, heads * width), kind),
            pltpu.SemaphoreType.DMA((3,)),
            pltpu.SemaphoreType.DMA((per_group,)),
            pltpu.SemaphoreType.DMA((per_group, groups)),
            pltpu.SemaphoreType.DMA((per_group, groups)),
            pltpu.SemaphoreType.DMA((per_group, blocks, groups)),
            pltpu.SemaphoreType.DMA((per_group, blocks, groups)),
            pltpu.SemaphoreType.DMA((per_group, groups)),
            pltpu.SemaphoreType.DMA((per_group, groups)),
            pltpu.SemaphoreType.DMA,
        ],
        compiler_params=pltpu.CompilerParams(collective_id=0, has_side_effects=True),
    )(queries, keys, values)


def solution(mesh):
    return jax.shard_map(
        shards,
        mesh=mesh,
        in_specs=(
            P(("dp", "sp"), None, None),
            P(("dp", "sp"), None, None),
            P(("dp", "sp"), None, None),
        ),
        out_specs=P(("dp", "sp"), None),
        check_vma=False,
    )
```

```python
import functools
import math

import jax
import jax.numpy as jnp
from jax import lax
from jax.experimental import pallas as pl
from jax.experimental.pallas import tpu as pltpu
from jax.sharding import PartitionSpec as P

HGROUPS = 8
MESH = pl.DeviceIdType.MESH


def order_of(group, groups):
    half = groups // 2
    side = group // half
    far = [(1 - side) * half + lax.rem(group + step, half) for step in range(half)]
    near = [side * half + lax.rem(group + step, half) for step in range(1, half)]
    return far + near


def kernel(
    groups, blocks, per_group,
    q_hbm, k_hbm, v_hbm, out_hbm,
    raw, wide, send, held, result, landed,
    in_sem, own_sem, send_sem, recv_sem, pass_sem, took_sem, back_sem, home_sem,
):
    me = lax.axis_index("sp")
    group, block = me // blocks, lax.rem(me, blocks)
    tokens, heads, width = q_hbm.shape
    half = groups // 2
    others = order_of(group, groups)
    partners = [lax.rem(block + step, blocks) for step in range(1, blocks)]

    loads = [
        pltpu.make_async_copy(src, raw.at[i], in_sem.at[i])
        for i, src in enumerate((q_hbm, k_hbm, v_hbm))
    ]
    for load in loads:
        load.start()

    barrier = pltpu.get_barrier_semaphore()
    for other in others:
        pl.semaphore_signal(barrier, inc=1, device_id={"sp": other * blocks + block}, device_id_type=MESH)
    for partner in partners:
        pl.semaphore_signal(barrier, inc=1, device_id={"sp": group * blocks + partner}, device_id_type=MESH)

    for i, load in enumerate(loads):
        load.wait()
        wide[i] = raw[i].astype(jnp.float32).reshape(tokens * heads, width)

    def outward(j, other):
        return pltpu.make_async_remote_copy(
            src_ref=send.at[other, j],
            dst_ref=held.at[j, block, group],
            send_sem=send_sem.at[j, other],
            recv_sem=recv_sem.at[j, group],
            device_id={"sp": other * blocks + block},
            device_id_type=MESH,
        )

    def inward(j, other):
        return pltpu.make_async_remote_copy(
            src_ref=send.at[other, j],
            dst_ref=held.at[j, block, other],
            send_sem=send_sem.at[j, other],
            recv_sem=recv_sem.at[j, other],
            device_id={"sp": other * blocks + block},
            device_id_type=MESH,
        )

    def own(j):
        return pltpu.make_async_copy(send.at[group, j], held.at[j, block, group], own_sem.at[j])

    def share(j, source, partner):
        part = held.at[j, block, source, pl.ds(1, 2)]
        return pltpu.make_async_remote_copy(
            src_ref=part,
            dst_ref=part,
            send_sem=pass_sem.at[j, partner, source],
            recv_sem=took_sem.at[j, block, source],
            device_id={"sp": group * blocks + partner},
            device_id_type=MESH,
        )

    def shared(j, source, partner):
        part = held.at[j, partner, source, pl.ds(1, 2)]
        return pltpu.make_async_remote_copy(
            src_ref=part,
            dst_ref=part,
            send_sem=pass_sem.at[j, partner, source],
            recv_sem=took_sem.at[j, partner, source],
            device_id={"sp": group * blocks + partner},
            device_id_type=MESH,
        )

    def columns(of, j):
        return pl.ds(pl.multiple_of((of * per_group + j) * width, width), width)

    def back(j, other):
        return pltpu.make_async_remote_copy(
            src_ref=result.at[j, other],
            dst_ref=landed.at[:, columns(group, j)],
            send_sem=back_sem.at[j, other],
            recv_sem=home_sem.at[j, group],
            device_id={"sp": other * blocks + block},
            device_id_type=MESH,
        )

    def home(j, other):
        return pltpu.make_async_remote_copy(
            src_ref=result.at[j, other],
            dst_ref=landed.at[:, columns(other, j)],
            send_sem=back_sem.at[j, other],
            recv_sem=home_sem.at[j, other],
            device_id={"sp": other * blocks + block},
            device_id_type=MESH,
        )

    def own_back(j):
        return pltpu.make_async_copy(
            result.at[j, group], landed.at[:, columns(group, j)], home_sem.at[j, group]
        )

    for j in range(per_group):
        for to in range(groups):
            head = to * per_group + j
            for i in range(3):
                rows = wide[i, pl.ds(head, tokens, stride=heads), :]
                send[to, j, i] = rows.astype(jnp.bfloat16)
        if j == 0:
            pl.semaphore_wait(barrier, groups - 1 + blocks - 1)
        for other in others:
            outward(j, other).start()
        own(j).start()

    factor = math.log2(math.e) / math.sqrt(width)
    for j in range(per_group):
        own(j).wait()
        for partner in partners:
            share(j, group, partner).start()
        for other in others:
            inward(j, other).wait_recv()
            for partner in partners:
                share(j, other, partner).start()
        for partner in partners:
            for source in [group] + others:
                shared(j, source, partner).wait_recv()
        keys = held[j, :, :, 1].reshape(-1, width)
        values = held[j, :, :, 2].reshape(-1, width)
        side = group // half
        for first, picked in (((1 - side) * half, others[:half]), (side * half, others[half:])):
            queries = held[j, block, pl.ds(first, half), 0].reshape(half * tokens, width)
            scores = lax.dot_general(
                queries, keys, (((1,), (1,)), ((), ())), preferred_element_type=jnp.float32
            )
            top = jnp.max(scores, axis=-1, keepdims=True)
            weights = jnp.exp2((scores - top) * factor)
            total = jnp.sum(weights, axis=-1, keepdims=True)
            attended = jnp.dot(
                weights.astype(jnp.bfloat16), values, preferred_element_type=jnp.float32
            ) / total
            result[j, pl.ds(first, half)] = attended.astype(jnp.bfloat16).reshape(half, tokens, width)
            for other in picked:
                back(j, other).start()
        own_back(j).start()

    for j in range(per_group):
        own_back(j).wait()
        for other in others:
            home(j, other).wait_recv()
    out_hbm[...] = landed[...]
    for j in range(per_group):
        for other in others:
            outward(j, other).wait_send()
            back(j, other).wait_send()
        for partner in partners:
            for source in [group] + others:
                share(j, source, partner).wait_send()


def shards(queries, keys, values):
    tokens, heads, width = queries.shape
    groups = HGROUPS
    blocks = lax.axis_size("sp") // groups
    per_group = heads // groups
    kind = queries.dtype
    return pl.pallas_call(
        functools.partial(kernel, groups, blocks, per_group),
        out_shape=pltpu.VMEM((tokens, heads * width), kind),
        in_specs=[pl.BlockSpec(memory_space=pl.ANY)] * 3,
        out_specs=pl.BlockSpec(memory_space=pltpu.VMEM),
        scratch_shapes=[
            pltpu.VMEM((3, tokens, heads, width), kind),
            pltpu.VMEM((3, tokens * heads, width), jnp.float32),
            pltpu.VMEM((groups, per_group, 3, tokens, width), kind),
            pltpu.VMEM((per_group, blocks, groups, 3, tokens, width), kind),
            pltpu.VMEM((per_group, groups, tokens, width), kind),
            pltpu.VMEM((tokens, heads * width), kind),
            pltpu.SemaphoreType.DMA((3,)),
            pltpu.SemaphoreType.DMA((per_group,)),
            pltpu.SemaphoreType.DMA((per_group, groups)),
            pltpu.SemaphoreType.DMA((per_group, groups)),
            pltpu.SemaphoreType.DMA((per_group, blocks, groups)),
            pltpu.SemaphoreType.DMA((per_group, blocks, groups)),
            pltpu.SemaphoreType.DMA((per_group, groups)),
            pltpu.SemaphoreType.DMA((per_group, groups)),
        ],
        compiler_params=pltpu.CompilerParams(collective_id=0, has_side_effects=True),
    )(queries, keys, values)


def solution(mesh):
    return jax.shard_map(
        shards,
        mesh=mesh,
        in_specs=(
            P(("dp", "sp"), None, None),
            P(("dp", "sp"), None, None),
            P(("dp", "sp"), None, None),
        ),
        out_specs=P(("dp", "sp"), None),
        check_vma=False,
    )
```

```python
import functools
import math

import jax
import jax.numpy as jnp
from jax import lax
from jax.experimental import pallas as pl
from jax.experimental.pallas import tpu as pltpu
from jax.sharding import PartitionSpec as P

HGROUPS = 8
MESH = pl.DeviceIdType.MESH


def order_of(group, groups):
    half = groups // 2
    side = group // half
    far = [(1 - side) * half + lax.rem(group + step, half) for step in range(half)]
    near = [side * half + lax.rem(group + step, half) for step in range(1, half)]
    return far, near


def ranked(group, groups):
    half = groups // 2
    side, place = group // half, lax.rem(group, half)
    far = [(1 - side) * half + step for step in range(half)]
    near = [side * half + step + (step + half - place) // half for step in range(half - 1)]
    return far, near


def kernel(
    groups, blocks, per_group,
    q_hbm, k_hbm, v_hbm, landed,
    raw, wide, send, held, result,
    in_sem, send_sem, recv_sem, pass_sem, took_sem, back_sem, home_sem,
):
    me = lax.axis_index("sp")
    group, block = me // blocks, lax.rem(me, blocks)
    tokens, heads, width = q_hbm.shape
    half = groups // 2
    side = group // half
    far, near = order_of(group, groups)
    partners = [lax.rem(block + step, blocks) for step in range(1, blocks)]

    loads = [
        pltpu.make_async_copy(src, raw.at[i], in_sem.at[i])
        for i, src in enumerate((q_hbm, k_hbm, v_hbm))
    ]
    for load in loads:
        load.start()

    barrier = pltpu.get_barrier_semaphore()
    for other in far + near:
        pl.semaphore_signal(barrier, inc=1, device_id={"sp": other * blocks + block}, device_id_type=MESH)
    for partner in partners:
        pl.semaphore_signal(barrier, inc=1, device_id={"sp": group * blocks + partner}, device_id_type=MESH)

    for i, load in enumerate(loads):
        load.wait()
        wide[i] = raw[i].astype(jnp.float32).reshape(tokens * heads, width)

    def outward(j, other, part):
        return pltpu.make_async_remote_copy(
            src_ref=send.at[other, j],
            dst_ref=held.at[j, block, group],
            send_sem=send_sem,
            recv_sem=recv_sem.at[j, part],
            device_id={"sp": other * blocks + block},
            device_id_type=MESH,
        )

    def own(j):
        return pltpu.make_async_copy(send.at[group, j], held.at[j, block, group], recv_sem.at[j, 0])

    def sources(part):
        return pl.ds((side if part == 0 else 1 - side) * half, half)

    def arrived(j, part):
        whole = held.at[j, block, sources(part)]
        pltpu.make_async_copy(whole, whole, recv_sem.at[j, part]).wait()

    def share(j, part, partner):
        piece = held.at[j, block, sources(part), pl.ds(1, 2)]
        return pltpu.make_async_remote_copy(
            src_ref=piece,
            dst_ref=piece,
            send_sem=pass_sem.at[partner],
            recv_sem=took_sem.at[j, block],
            device_id={"sp": group * blocks + partner},
            device_id_type=MESH,
        )

    def shared(j, partner):
        whole = held.at[j, partner, :, pl.ds(1, 2)]
        pltpu.make_async_copy(whole, whole, took_sem.at[j, partner]).wait()

    def columns(of, j):
        return pl.ds(pl.multiple_of((of * per_group + j) * width, width), width)

    def back(j, other):
        return pltpu.make_async_remote_copy(
            src_ref=result.at[j, other],
            dst_ref=landed.at[:, columns(group, j)],
            send_sem=back_sem,
            recv_sem=home_sem,
            device_id={"sp": other * blocks + block},
            device_id_type=MESH,
        )

    def own_back(j):
        return pltpu.make_async_copy(result.at[j, group], landed.at[:, columns(group, j)], home_sem)

    for j in range(per_group):
        for to in range(groups):
            head = to * per_group + j
            for i in range(3):
                rows = wide[i, pl.ds(head, tokens, stride=heads), :]
                send[to, j, i] = rows.astype(jnp.bfloat16)
        if j == 0:
            pl.semaphore_wait(barrier, groups - 1 + blocks - 1)
        for other in far:
            outward(j, other, 1).start()
        for other in near:
            outward(j, other, 0).start()
        own(j).start()

    factor = math.log2(math.e) / math.sqrt(width)
    far, near = ranked(group, groups)
    for j in range(per_group):
        for part in range(2):
            arrived(j, part)
            for partner in partners:
                share(j, part, partner).start()
        for partner in partners:
            shared(j, partner)
        keys = held[j, :, :, 1].reshape(-1, width)
        values = held[j, :, :, 2].reshape(-1, width)
        for first, picked in (((1 - side) * half, far), (side * half, near)):
            queries = held[j, block, pl.ds(first, half), 0].reshape(half * tokens, width)
            scores = lax.dot_general(
                queries, keys, (((1,), (1,)), ((), ())), preferred_element_type=jnp.float32
            )
            top = jnp.max(scores, axis=-1, keepdims=True)
            weights = jnp.exp2((scores - top) * factor)
            total = jnp.sum(weights, axis=-1, keepdims=True)
            attended = jnp.dot(
                weights.astype(jnp.bfloat16), values, preferred_element_type=jnp.float32
            ) / total
            result[j, pl.ds(first, half)] = attended.astype(jnp.bfloat16).reshape(half, tokens, width)
            for other in picked:
                back(j, other).start()
        own_back(j).start()

    sent = send.at[pl.ds(0, groups - 1)]
    pltpu.make_async_copy(sent, sent, send_sem).wait()
    for partner in partners:
        passed = held.at[:, block, :, pl.ds(1, 2)]
        pltpu.make_async_copy(passed, passed, pass_sem.at[partner]).wait()
    given = result.at[:, pl.ds(0, groups - 1)]
    pltpu.make_async_copy(given, given, back_sem).wait()
    pltpu.make_async_copy(landed, landed, home_sem).wait()


def shards(queries, keys, values):
    tokens, heads, width = queries.shape
    groups = HGROUPS
    blocks = lax.axis_size("sp") // groups
    per_group = heads // groups
    kind = queries.dtype
    return pl.pallas_call(
        functools.partial(kernel, groups, blocks, per_group),
        out_shape=pltpu.VMEM((tokens, heads * width), kind),
        in_specs=[pl.BlockSpec(memory_space=pl.ANY)] * 3,
        out_specs=pl.BlockSpec(memory_space=pltpu.VMEM),
        scratch_shapes=[
            pltpu.VMEM((3, tokens, heads, width), kind),
            pltpu.VMEM((3, tokens * heads, width), jnp.float32),
            pltpu.VMEM((groups, per_group, 3, tokens, width), kind),
            pltpu.VMEM((per_group, blocks, groups, 3, tokens, width), kind),
            pltpu.VMEM((per_group, groups, tokens, width), kind),
            pltpu.SemaphoreType.DMA((3,)),
            pltpu.SemaphoreType.DMA,
            pltpu.SemaphoreType.DMA((per_group, 2)),
            pltpu.SemaphoreType.DMA((blocks,)),
            pltpu.SemaphoreType.DMA((per_group, blocks)),
            pltpu.SemaphoreType.DMA,
            pltpu.SemaphoreType.DMA,
        ],
        compiler_params=pltpu.CompilerParams(collective_id=0, has_side_effects=True),
    )(queries, keys, values)


def solution(mesh):
    return jax.shard_map(
        shards,
        mesh=mesh,
        in_specs=(
            P(("dp", "sp"), None, None),
            P(("dp", "sp"), None, None),
            P(("dp", "sp"), None, None),
        ),
        out_specs=P(("dp", "sp"), None),
        check_vma=False,
    )
```

```python
import functools
import math

import jax
import jax.numpy as jnp
from jax import lax
from jax.experimental import pallas as pl
from jax.experimental.pallas import tpu as pltpu
from jax.sharding import PartitionSpec as P

HGROUPS = 8
MESH = pl.DeviceIdType.MESH


def order_of(group, groups):
    half = groups // 2
    side = group // half
    far = [(1 - side) * half + lax.rem(group + step, half) for step in range(half)]
    near = [side * half + lax.rem(group + step, half) for step in range(1, half)]
    return far, near


def ranked(group, groups):
    half = groups // 2
    side, place = group // half, lax.rem(group, half)
    far = [(1 - side) * half + step for step in range(half)]
    near = [side * half + step + (step + half - place) // half for step in range(half - 1)]
    return far, near


def kernel(
    groups, blocks, per_group,
    q_hbm, k_hbm, v_hbm, landed,
    raw, wide, send, held, result,
    in_sem, send_sem, recv_sem, pass_sem, took_sem, back_sem, home_sem,
):
    me = lax.axis_index("sp")
    group, block = me // blocks, lax.rem(me, blocks)
    tokens, heads, width = q_hbm.shape
    half = groups // 2
    side = group // half
    far, near = order_of(group, groups)
    partners = [lax.rem(block + step, blocks) for step in range(1, blocks)]

    loads = [
        pltpu.make_async_copy(src, raw.at[i], in_sem.at[i])
        for i, src in enumerate((q_hbm, k_hbm, v_hbm))
    ]
    for load in loads:
        load.start()

    barrier = pltpu.get_barrier_semaphore()
    for other in far + near:
        pl.semaphore_signal(barrier, inc=1, device_id={"sp": other * blocks + block}, device_id_type=MESH)
    for partner in partners:
        pl.semaphore_signal(barrier, inc=1, device_id={"sp": group * blocks + partner}, device_id_type=MESH)

    for i, load in enumerate(loads):
        load.wait()
        wide[i] = raw[i].astype(jnp.float32).reshape(tokens * heads, width)

    def outward(j, other, part):
        return pltpu.make_async_remote_copy(
            src_ref=send.at[other, j],
            dst_ref=held.at[j, block, group],
            send_sem=send_sem,
            recv_sem=recv_sem.at[j, part],
            device_id={"sp": other * blocks + block},
            device_id_type=MESH,
        )

    def own(j):
        return pltpu.make_async_copy(send.at[group, j], held.at[j, block, group], recv_sem.at[j, 0])

    def sources(part):
        return pl.ds((side if part == 0 else 1 - side) * half, half)

    def arrived(j, part):
        whole = held.at[j, block, sources(part)]
        pltpu.make_async_copy(whole, whole, recv_sem.at[j, part]).wait()

    def share(j, part, partner):
        piece = held.at[j, block, sources(part), pl.ds(1, 2)]
        return pltpu.make_async_remote_copy(
            src_ref=piece,
            dst_ref=piece,
            send_sem=pass_sem.at[partner],
            recv_sem=took_sem.at[j, block],
            device_id={"sp": group * blocks + partner},
            device_id_type=MESH,
        )

    def shared(j, partner):
        whole = held.at[j, partner, :, pl.ds(1, 2)]
        pltpu.make_async_copy(whole, whole, took_sem.at[j, partner]).wait()

    def columns(of, j):
        return pl.ds(pl.multiple_of((of * per_group + j) * width, width), width)

    def back(j, other):
        return pltpu.make_async_remote_copy(
            src_ref=result.at[j, other],
            dst_ref=landed.at[:, columns(group, j)],
            send_sem=back_sem,
            recv_sem=home_sem,
            device_id={"sp": other * blocks + block},
            device_id_type=MESH,
        )

    def own_back(j):
        return pltpu.make_async_copy(result.at[j, group], landed.at[:, columns(group, j)], home_sem)

    for j in range(per_group):
        for to in range(groups):
            head = to * per_group + j
            for i in range(3):
                rows = wide[i, pl.ds(head, tokens, stride=heads), :]
                send[to, j, i] = rows.astype(jnp.bfloat16)
        if j == 0:
            pl.semaphore_wait(barrier, groups - 1 + blocks - 1)
        for other in far:
            outward(j, other, 1).start()
        for other in near:
            outward(j, other, 0).start()
        own(j).start()

    factor = math.log2(math.e) / math.sqrt(width)
    far, near = ranked(group, groups)
    for j in range(per_group):
        for part in range(2):
            arrived(j, part)
            for partner in partners:
                share(j, part, partner).start()
        for partner in partners:
            shared(j, partner)
        keys = held[j, :, :, 1].reshape(-1, width)
        values = held[j, :, :, 2].reshape(-1, width)
        if j == per_group - 1:
            @pl.when(side == 0)
            def release():
                for earlier in (1,):
                    for other in far:
                        back(earlier, other).start()

        for first, picked in (((1 - side) * half, far), (side * half, near)):
            queries = held[j, block, pl.ds(first, half), 0].reshape(half * tokens, width)
            scores = lax.dot_general(
                queries, keys, (((1,), (1,)), ((), ())), preferred_element_type=jnp.float32
            )
            top = jnp.max(scores, axis=-1, keepdims=True)
            weights = jnp.exp2((scores - top) * factor)
            total = jnp.sum(weights, axis=-1, keepdims=True)
            attended = jnp.dot(
                weights.astype(jnp.bfloat16), values, preferred_element_type=jnp.float32
            ) / total
            result[j, pl.ds(first, half)] = attended.astype(jnp.bfloat16).reshape(half, tokens, width)
            if picked is far and j in (1,):
                @pl.when(side > 0)
                def forward():
                    for other in picked:
                        back(j, other).start()
            else:
                for other in picked:
                    back(j, other).start()
        own_back(j).start()

    sent = send.at[pl.ds(0, groups - 1)]
    pltpu.make_async_copy(sent, sent, send_sem).wait()
    for partner in partners:
        passed = held.at[:, block, :, pl.ds(1, 2)]
        pltpu.make_async_copy(passed, passed, pass_sem.at[partner]).wait()
    given = result.at[:, pl.ds(0, groups - 1)]
    pltpu.make_async_copy(given, given, back_sem).wait()
    pltpu.make_async_copy(landed, landed, home_sem).wait()


def shards(queries, keys, values):
    tokens, heads, width = queries.shape
    groups = HGROUPS
    blocks = lax.axis_size("sp") // groups
    per_group = heads // groups
    kind = queries.dtype
    return pl.pallas_call(
        functools.partial(kernel, groups, blocks, per_group),
        out_shape=pltpu.VMEM((tokens, heads * width), kind),
        in_specs=[pl.BlockSpec(memory_space=pl.ANY)] * 3,
        out_specs=pl.BlockSpec(memory_space=pltpu.VMEM),
        scratch_shapes=[
            pltpu.VMEM((3, tokens, heads, width), kind),
            pltpu.VMEM((3, tokens * heads, width), jnp.float32),
            pltpu.VMEM((groups, per_group, 3, tokens, width), kind),
            pltpu.VMEM((per_group, blocks, groups, 3, tokens, width), kind),
            pltpu.VMEM((per_group, groups, tokens, width), kind),
            pltpu.SemaphoreType.DMA((3,)),
            pltpu.SemaphoreType.DMA,
            pltpu.SemaphoreType.DMA((per_group, 2)),
            pltpu.SemaphoreType.DMA((blocks,)),
            pltpu.SemaphoreType.DMA((per_group, blocks)),
            pltpu.SemaphoreType.DMA,
            pltpu.SemaphoreType.DMA,
        ],
        compiler_params=pltpu.CompilerParams(collective_id=0, has_side_effects=True),
    )(queries, keys, values)


def solution(mesh):
    return jax.shard_map(
        shards,
        mesh=mesh,
        in_specs=(
            P(("dp", "sp"), None, None),
            P(("dp", "sp"), None, None),
            P(("dp", "sp"), None, None),
        ),
        out_specs=P(("dp", "sp"), None),
        check_vma=False,
    )
```
